32 devices in a mesh: pair: 8 (over z, x), sector: 4 (over y, core).
Axes of the slice: x: 2, y: 2, z: 4, core: 2. Of those that a mesh axis runs over, the one named last changes fastest.
Arguments:
- wave: bfloat16 [4, 1024, 1024], P('sector', 'pair'), may hold values from -6 to 6
- left_ops: bfloat16 [16, 4, 1024, 1024], P('pair', 'sector'), may hold values from -0.1875 to 0.1875
- right_ops: bfloat16 [16, 4, 1024, 1024], P('pair', 'sector'), may hold values from -0.046875 to 0.046875
- targets: int32 [16, 4], P('pair', 'sector'), may hold values from -1 to 3
- sector_sizes: int32 [4], replicated, may hold values from 256 to 1024
- pair_ids: int32 [16], P('pair'), may hold values from 0 to 15, each once
- pair_coefficients: float32 [16], replicated, may hold values from 0.25 to 2
Outputs:
- sigma_blocks: float32 [4, 1024, 1024], P('sector', 'pair')
The draws below stay inside these ranges and needn't reach their ends.
Inputs may be any that keep to these rules, and one draw needn't show every extreme that they name: `pair_ids`: each orbital pair once.
All inputs are finite; a program needn't handle non-finite values.
Results may differ from the reference program's by a relative error of at most 0.0029.
Values may be sent and summed in bfloat16 or wider, within the bound.
A program may use at most 128 MiB of HBM per device.

```python
import math
import jax
import jax.numpy as jnp
from jax import lax

BLOCK = 1024
SECTORS = 4
PAIRS = 16


def set_ends(values, own_key, low, largest):
    longest = values.shape.index(max(values.shape))
    spots = []
    for shift in (0, 1):
        where = [jax.random.randint(jax.random.fold_in(own_key, axis), (), 0, length) for axis, length in enumerate(values.shape)]
        where[longest] = (where[longest] + shift) % values.shape[longest]
        spots.append(tuple(where))
    return values.at[spots[0]].set(low).at[spots[1]].set(largest)


def levels(key, dims, cuts, low, top_value):
    gain = 1.0
    for axis_at, parts in cuts:
        heights = jax.random.uniform(jax.random.fold_in(jax.random.fold_in(key, 6), axis_at), (parts,), jnp.float32, low / len(cuts), top_value / len(cuts))
        gain = gain * jnp.repeat(jnp.exp(heights), dims[axis_at] // parts).reshape((-1,) + (1,) * (len(dims) - 1 - axis_at))
    return gain


def normal_values(rng, shape, deviation, reach, shards=(), held_as=jnp.bfloat16):
    level = levels(rng, shape, shards, -0.22, 0.18) if shards else 1.0
    values = jax.random.normal(rng, shape, jnp.float32) * deviation * level
    return jnp.minimum(jnp.maximum(values, -reach), reach).astype(held_as)


def setup_inputs(seed: int = 0) -> dict:
    arg_keys = jax.random.split(jax.random.key(seed), 8)
    return {
        "wave": normal_values(arg_keys[0], (SECTORS, BLOCK, BLOCK), 1.0, 6.0, ((0, 4), (1, 8))),
        "left_ops": normal_values(arg_keys[1], (PAIRS, SECTORS, BLOCK, BLOCK), BLOCK ** -0.5, 0.1875, ((0, 8), (1, 4))),
        "right_ops": normal_values(arg_keys[2], (PAIRS, SECTORS, BLOCK, BLOCK), (BLOCK * PAIRS) ** -0.5, 0.046875, ((0, 8), (1, 4))),
        "targets": set_ends(jax.random.randint(arg_keys[3], (PAIRS, SECTORS), -1, SECTORS), jax.random.fold_in(arg_keys[3], 1), -1, SECTORS - 1).astype(jnp.int32),
        "sector_sizes": set_ends(jax.random.randint(arg_keys[4], (SECTORS,), BLOCK // 4, BLOCK + 1), jax.random.fold_in(arg_keys[4], 1), BLOCK // 4, BLOCK).astype(jnp.int32),
        "pair_ids": jax.random.permutation(arg_keys[5], PAIRS).astype(jnp.int32),
        "pair_coefficients": jnp.clip(jnp.exp(jax.random.uniform(arg_keys[6], (PAIRS,), jnp.float32, math.log(0.25), math.log(2.0))), 0.25, 2.0),
    }


def reference(wave, left_ops, right_ops, targets, sector_sizes, pair_ids, pair_coefficients):
    positions = jnp.arange(BLOCK, dtype=jnp.int32)
    used = (positions[None, :] < sector_sizes[:, None]).astype(wave.dtype)
    masked = wave * used[:, :, None] * used[:, None, :]
    factor = pair_coefficients[pair_ids]
    sector_ids = jnp.arange(SECTORS, dtype=jnp.int32)

    def one_pair(totals, packed):
        left_op, right_op, target, weight = packed
        for source in range(SECTORS):
            left = jnp.dot(left_op[source], masked[source], preferred_element_type=jnp.float32).astype(jnp.bfloat16)
            term = lax.dot_general(left, right_op[source], (((1,), (1,)), ((), ())), preferred_element_type=jnp.float32)
            chosen = (sector_ids == target[source]).astype(jnp.float32)
            totals = totals + chosen[:, None, None] * (weight * term)[None]
        return totals, None

    start_totals = jnp.zeros((SECTORS, BLOCK, BLOCK), jnp.float32)
    totals, _ = lax.scan(one_pair, start_totals, (left_ops, right_ops, targets, factor))
    used_float = used.astype(jnp.float32)
    return totals * used_float[:, :, None] * used_float[:, None, :]
```

```python
import functools

import jax
import jax.numpy as jnp
from jax import lax
from jax.experimental import pallas as pl
from jax.experimental.pallas import tpu as pltpu
from jax.sharding import PartitionSpec as P

MESH = pl.DeviceIdType.MESH
F32 = jnp.float32
LANES = 128
PLANE_DEPTH = 128
ROW_TILE = 256


def step_kernel(
    cfg, wave_ref, weight_ref, left_hbm, right_hbm, out_ref,
    wbuf, lbuf, rbuf, acc, left, own, psend, precv, wother,
    xs, xr, ys, yr, zs, zup, zdn, fsend, frecv, load_sem, sems_s, sems_r, line_s, line_r, gat_s, gat_r,
):
    Z, X, T, K, rows, block, groups, orders = cfg
    half = block // 2
    pair, sector = lax.axis_index("pair"), lax.axis_index("sector")
    z, x = pair // X, lax.rem(pair, X)
    y, c = sector // 2, lax.rem(sector, 2)

    def dev(zz=None, xx=None, yy=None, cc=None):
        zz, xx = z if zz is None else zz, x if xx is None else xx
        yy, cc = y if yy is None else yy, c if cc is None else cc
        return (zz * X + xx, yy * 2 + cc)

    x_dev, y_dev, c_dev = dev(xx=1 - x), dev(yy=1 - y), dev(cc=1 - c)
    up_dev, dn_dev = dev(zz=z + 1), dev(zz=z - 1)
    has_up, has_dn = z + 1 < Z, z >= 1

    loads = []
    for k in range(K):
        loads.append(pltpu.make_async_copy(left_hbm.at[k], lbuf.at[k], load_sem.at[k]))
        loads.append(pltpu.make_async_copy(right_hbm.at[k], rbuf.at[k], load_sem.at[K + k]))
    for k in range(K):
        loads[2 * k].start()

    barrier = pltpu.get_barrier_semaphore()
    for other in (x_dev, y_dev, c_dev):
        pl.semaphore_signal(barrier, inc=1, device_id=other, device_id_type=MESH)

    @pl.when(has_up)
    def _():
        pl.semaphore_signal(barrier, inc=1, device_id=up_dev, device_id_type=MESH)

    @pl.when(has_dn)
    def _():
        pl.semaphore_signal(barrier, inc=1, device_id=dn_dev, device_id_type=MESH)

    pl.semaphore_wait(barrier, 3 + has_up.astype(jnp.int32) + has_dn.astype(jnp.int32))

    def remote(src, dst, ss, rs, device):
        return pltpu.make_async_remote_copy(
            src_ref=src, dst_ref=dst, send_sem=ss, recv_sem=rs, device_id=device, device_id_type=MESH
        )

    def hop(q, way, src=None):
        device = (up_dev, dn_dev, x_dev)[way]
        src = wbuf.at[q, x] if src is None else src
        return remote(src, wbuf.at[q, x], gat_s.at[way, q], gat_r.at[q, x], device)

    def arrival(q, xx):
        return remote(wbuf.at[q, xx], wbuf.at[q, xx], gat_s.at[2, q], gat_r.at[q, xx], x_dev)

    @pl.when(has_up)
    def _():
        hop(z, 0, wave_ref).start()

    @pl.when(has_dn)
    def _():
        hop(z, 1, wave_ref).start()

    hop(z, 2, wave_ref).start()
    weights_copy = remote(weight_ref, wother, sems_s.at[0], sems_r.at[0], c_dev)
    weights_copy.start()
    for k in range(K):
        loads[2 * k + 1].start()

    for g in range(groups):
        @pl.when(jnp.logical_not(has_dn))
        def _(g=g):
            zup[g][z] = jnp.zeros(zup[g].shape[1:], zup[g].dtype)

        @pl.when(jnp.logical_not(has_up))
        def _(g=g):
            zdn[g][z] = jnp.zeros(zdn[g].shape[1:], zdn[g].dtype)

    depth = X * rows
    planewise = depth % PLANE_DEPTH == 0
    tile = min(ROW_TILE, block)
    tiles = block // tile

    def multiply(q, first):
        plane = wbuf.at[q]

        def one(i, carry):
            k, at = i // tiles, pl.multiple_of(lax.rem(i, tiles) * tile, tile)
            cols = pl.ds(pl.multiple_of(q * depth, depth), depth)
            product = jnp.dot(
                lbuf[k, pl.ds(at, tile), cols], plane[...].reshape(depth, block), preferred_element_type=F32
            )
            if first:
                acc[k, pl.ds(at, tile), :] = product
            else:
                acc[k, pl.ds(at, tile), :] += product
            return carry

        lax.fori_loop(0, K * tiles, one, 0)

    def take_plane(q):
        arrival(q, 1 - x).wait_recv()
        if planewise:
            multiply(q, False)

    wbuf[z, x] = wave_ref[...]
    for k in range(K):
        loads[2 * k].wait()

    def forward(d, carry):
        lo, hi = z - d, z + d

        @pl.when(lo >= 0)
        def _():
            arrival(lo, x).wait_recv()

            @pl.when(has_up)
            def _():
                hop(lo, 0).start()

            hop(lo, 2).start()

        @pl.when(hi < Z)
        def _():
            arrival(hi, x).wait_recv()

            @pl.when(has_dn)
            def _():
                hop(hi, 1).start()

            hop(hi, 2).start()

        @pl.when(d == 1)
        def _():
            arrival(z, 1 - x).wait_recv()
            if planewise:
                multiply(z, True)

        @pl.when(jnp.logical_and(d > 1, lo + 1 >= 0))
        def _():
            take_plane(lo + 1)

        @pl.when(jnp.logical_and(d > 1, hi - 1 < Z))
        def _():
            take_plane(hi - 1)

        return carry

    lax.fori_loop(1, Z, forward, 0)

    @pl.when(z == Z - 1)
    def _():
        take_plane(0)

    @pl.when(z == 0)
    def _():
        take_plane(Z - 1)

    def finish_left(i, carry):
        k, at = i // tiles, pl.multiple_of(lax.rem(i, tiles) * tile, tile)
        if planewise:
            value = acc[k, pl.ds(at, tile), :]
        else:
            value = jnp.dot(
                lbuf[k, pl.ds(at, tile), :], wbuf[...].reshape(block, block), preferred_element_type=F32
            )
        left[k, pl.ds(at, tile), :] = value.astype(jnp.bfloat16)
        return carry

    lax.fori_loop(0, K * tiles, finish_left, 0)
    for k in range(K):
        loads[2 * k + 1].wait()

    width = 2 * LANES

    def second(part, side, dest):
        def one(i, carry):
            k, at = i // tiles, pl.multiple_of(lax.rem(i, tiles) * tile, tile)
            right_at = pl.multiple_of(side * half + part * width, width)
            term = lax.dot_general(
                left[k, pl.ds(at, tile), :], rbuf[k, pl.ds(right_at, width), :],
                (((1,), (1,)), ((), ())), preferred_element_type=F32,
            )
            for j in range(2):
                dest[2 * part + j, k, pl.ds(at, tile), :] = term[:, j * LANES : (j + 1) * LANES].astype(dest.dtype)
            return carry

        lax.fori_loop(0, K * tiles, one, 0)

    def part_copy(part):
        span = pl.ds(2 * part, 2)
        return remote(psend.at[span], precv.at[span], sems_s.at[1 + part], sems_r.at[1 + part], c_dev)

    base = 1 + groups // 2

    def step_copy(g, number):
        letter = orders[g].replace("z", "")[number]
        s, r = ((xs, xr), (ys, yr))["xy".index(letter)]
        at = base + 2 * g + number
        return remote(s[g], r[g], sems_s.at[at], sems_r.at[at], x_dev if letter == "x" else y_dev)

    def chip_sum(g, ty, tc, zz, xx):
        at = pl.ds(pl.multiple_of((zz * X + xx) * rows, rows), rows)
        t = ty * 2 + tc
        total = None
        for k in range(K):
            mine = own[g, k, at, :] * weight_ref[k * T + t, 0:1, :]
            theirs = precv[g, k, at, :].astype(F32) * wother[k * T + t, 0:1, :]
            total = mine + theirs if total is None else total + mine + theirs
        return total

    def loop(count, f):
        def one(i, carry):
            f(i)
            return carry

        lax.fori_loop(0, count, one, 0)

    def x_first(g):
        def one(zz):
            for ty in range(2):
                for tc in range(2):
                    xs[g][ty, tc, zz] = chip_sum(g, ty, tc, zz, 1 - x).astype(jnp.bfloat16)
        loop(Z, one)
        step_copy(g, 0).start()

    def y_first(g):
        def one(zz):
            for tc in range(2):
                for xx in range(2):
                    ys[g][tc, zz, xx] = chip_sum(g, 1 - y, tc, zz, xx).astype(jnp.bfloat16)
        loop(Z, one)
        step_copy(g, 0).start()

    def y_second(g):
        step_copy(g, 0).wait_recv()

        def one(zz):
            for tc in range(2):
                value = chip_sum(g, 1 - y, tc, zz, x) + xr[g][1 - y, tc, zz].astype(F32)
                ys[g][tc, zz] = value.astype(jnp.bfloat16)
        loop(Z, one)
        step_copy(g, 1).start()

    def x_second(g):
        step_copy(g, 0).wait_recv()

        def one(zz):
            for tc in range(2):
                value = chip_sum(g, y, tc, zz, 1 - x) + yr[g][tc, zz, 1 - x].astype(F32)
                xs[g][tc, zz] = value.astype(jnp.bfloat16)
        loop(Z, one)
        step_copy(g, 1).start()

    def line_item(g, tc, zz):
        value = chip_sum(g, y, tc, zz, x)
        if orders[g][0] == "x":
            return value + xr[g][y, tc, zz].astype(F32) + yr[g][tc, zz].astype(F32)
        return value + yr[g][tc, zz, x].astype(F32) + xr[g][tc, zz].astype(F32)

    def line_values(g, zz):
        return {(tc,): line_item(g, tc, zz) for tc in range(2)}

    def line_copy(g, zz, way):
        dst = (zup, zdn)[way][g].at[zz]
        return remote(zs[g].at[zz], dst, line_s.at[g, zz], line_r.at[g, way, zz], (up_dev, dn_dev)[way])

    def line_step(g, j):
        for way, zz, active, middle in ((0, Z - 1 - j, Z - 1 - j > z, has_dn), (1, j, j < z, has_up)):
            @pl.when(active)
            def _(way=way, zz=zz, middle=middle):
                @pl.when(middle)
                def _():
                    line_copy(g, zz, way).wait_recv()
                    for at, value in line_values(g, zz).items():
                        arrived = (zup, zdn)[way][g][(zz,) + at]
                        zs[g][(zz,) + at] = (value + arrived.astype(F32)).astype(zs[g].dtype)

                @pl.when(jnp.logical_not(middle))
                def _():
                    for at, value in line_values(g, zz).items():
                        zs[g][(zz,) + at] = value.astype(zs[g].dtype)

                line_copy(g, zz, way).start()

    def line_all(chosen):
        loop(Z - 1, lambda j: [line_step(g, j) for g in chosen])

    def line_end(g):
        @pl.when(has_dn)
        def _():
            line_copy(g, z, 0).wait_recv()

        @pl.when(has_up)
        def _():
            line_copy(g, z, 1).wait_recv()

    def ended(g, at, value):
        return value + zup[g][(z,) + at].astype(F32) + zdn[g][(z,) + at].astype(F32)

    def final_copy(g):
        at = base + 2 * groups + g
        return remote(fsend.at[g], frecv.at[g], sems_s.at[at], sems_r.at[at], c_dev)

    def finish(g):
        def value(tc):
            return ended(g, (tc,), line_item(g, tc, z))

        line_end(g)
        fsend[g] = value(1 - c)
        final_copy(g).start()
        out_ref[c, g] = value(c)

    for part in range(groups // 2):
        second(part, 1 - c, psend)
        part_copy(part).start()
        second(part, c, own)
        if part == 0:
            weights_copy.wait_recv()
        part_copy(part).wait_recv()
        x_first(2 * part)
        y_first(2 * part + 1)
    def lines(part):
        for g in (2 * part, 2 * part + 1):
            step_copy(g, 1).wait_recv()
        line_all((2 * part, 2 * part + 1))

    for part in range(groups // 2):
        y_second(2 * part)
        x_second(2 * part + 1)
        if part:
            lines(part - 1)
    lines(groups // 2 - 1)
    for g in range(groups):
        finish(g)
    for g in range(groups):
        final_copy(g).wait_recv()
    out_ref[1 - c] = frecv[...]

    for q_way in range(3):
        def drain(q, q_way=q_way):
            sent = (
                jnp.logical_and(has_up, q <= z),
                jnp.logical_and(has_dn, q >= z),
                None,
            )[q_way]
            if sent is None:
                hop(q, q_way).wait_send()
            else:
                @pl.when(sent)
                def _():
                    hop(q, q_way).wait_send()
        loop(Z, drain)
    weights_copy.wait_send()
    for part in range(groups // 2):
        part_copy(part).wait_send()
    for g in range(groups):
        step_copy(g, 0).wait_send()
        step_copy(g, 1).wait_send()
        final_copy(g).wait_send()

        def drain_line(zz, g=g):
            @pl.when(zz > z)
            def _():
                line_copy(g, zz, 0).wait_send()

            @pl.when(zz < z)
            def _():
                line_copy(g, zz, 1).wait_send()
        loop(Z, drain_line)


def kernel_entry(cfg, *refs):
    groups = cfg[6]
    ins, scratch = refs[:5], list(refs[5:])
    plain = scratch[:9]
    per_group = [scratch[9 + n * groups : 9 + (n + 1) * groups] for n in range(7)]
    step_kernel(cfg, *ins, *plain, *per_group, *scratch[9 + 7 * groups :])


def body(wave, left_ops, right_ops, targets, sector_sizes, pair_ids, pair_coefficients):
    block = wave.shape[2]
    rows = wave.shape[1]
    K = left_ops.shape[0]
    T = sector_sizes.shape[0]
    pairs = lax.axis_size("pair")
    X = 2
    Z = pairs // X
    half = block // 2
    groups = half // LANES
    orders = tuple(("xyz", "yxz")[g % 2] for g in range(groups))
    own_sector = lax.axis_index("sector")
    sector_ids = jnp.arange(T, dtype=jnp.int32)
    own_size = jnp.sum(jnp.where(sector_ids == own_sector, sector_sizes, 0))
    col_ids = jnp.arange(block, dtype=jnp.int32)
    row_ids = lax.axis_index("pair") * rows + jnp.arange(rows, dtype=jnp.int32)
    used = (row_ids < own_size)[:, None] & (col_ids < own_size)[None, :]
    masked = wave[0] * used.astype(wave.dtype)
    table_ids = jnp.arange(pair_coefficients.shape[0], dtype=jnp.int32)
    factor = jnp.sum(
        jnp.where(pair_ids[:, None] == table_ids[None, :], pair_coefficients[None, :], 0.0), axis=1
    )
    weights = jnp.where(targets == sector_ids[None, :], factor[:, None], 0.0).reshape(K * T, 1, 1)
    weights = jnp.broadcast_to(weights, (K * T, 8, LANES)).astype(F32)

    bf = jnp.bfloat16
    line_type = bf if Z <= 4 else F32
    xs, xr, ys, yr, zs, zup, zdn = [], [], [], [], [], [], []
    for order in orders:
        tail = (rows, LANES)
        x_shape, y_shape, z_shape = {
            "x": ((2, 2, Z), (2, Z), (Z, 2)),
            "y": ((2, Z), (2, Z, X), (Z, 2)),
        }[order[0]]
        for where, shape, kind in (
            (xs, x_shape, bf), (xr, x_shape, bf), (ys, y_shape, bf), (yr, y_shape, bf),
            (zs, z_shape, line_type), (zup, z_shape, line_type), (zdn, z_shape, line_type),
        ):
            where.append(pltpu.VMEM(shape + tail, kind))
    count = 1 + groups // 2 + 3 * groups
    dma = pltpu.SemaphoreType.DMA
    cfg = (Z, X, T, K, rows, block, groups, orders)
    planewise = (X * rows) % PLANE_DEPTH == 0
    vmem, anywhere = pl.BlockSpec(memory_space=pltpu.VMEM), pl.BlockSpec(memory_space=pl.ANY)
    parts = pl.pallas_call(
        functools.partial(kernel_entry, cfg),
        out_shape=jax.ShapeDtypeStruct((2, groups, rows, LANES), F32),
        in_specs=[vmem, vmem, anywhere, anywhere],
        out_specs=vmem,
        scratch_shapes=[
            pltpu.VMEM((Z, X, rows, block), bf),
            pltpu.VMEM((K, block, block), bf),
            pltpu.VMEM((K, block, block), bf),
            pltpu.VMEM((K, block, block) if planewise else (8, LANES), F32),
            pltpu.VMEM((K, block, block), bf),
            pltpu.VMEM((groups, K, block, LANES), F32),
            pltpu.VMEM((groups, K, block, LANES), F32),
            pltpu.VMEM((groups, K, block, LANES), F32),
            pltpu.VMEM((K * T, 8, LANES), F32),
            *xs, *xr, *ys, *yr, *zs, *zup, *zdn,
            pltpu.VMEM((groups, rows, LANES), F32),
            pltpu.VMEM((groups, rows, LANES), F32),
            dma((2 * K,)), dma((count,)), dma((count,)),
            dma((groups, Z)), dma((groups, 2, Z)), dma((3, Z)), dma((Z, X)),
        ],
        compiler_params=pltpu.CompilerParams(
            collective_id=0, has_side_effects=True, vmem_limit_bytes=60 * 1024 * 1024
        ),
        name="sigma_step",
    )(masked, weights, left_ops[:, 0], right_ops[:, 0])
    summed = parts.transpose(2, 0, 1, 3).reshape(rows, block)
    return (summed * used.astype(F32))[None]


def solution(mesh):
    placed = (
        P("sector", "pair", None),
        P("pair", "sector", None, None),
        P("pair", "sector", None, None),
        P("pair", "sector"),
        P(),
        P("pair"),
        P(),
    )
    return jax.shard_map(
        body, mesh=mesh, in_specs=placed, out_specs=P("sector", "pair", None), check_vma=False
    )
```

```python
import functools

import jax
import jax.numpy as jnp
from jax import lax
from jax.experimental import pallas as pl
from jax.experimental.pallas import tpu as pltpu
from jax.sharding import PartitionSpec as P

MESH = pl.DeviceIdType.MESH
F32 = jnp.float32
LANES = 128
PLANE_DEPTH = 128
ROW_TILE = 256
PIECES = 2


def step_kernel(
    cfg, wave_ref, targets_ref, sizes_ref, ids_ref, coefs_ref, left_hbm, right_hbm, out_ref,
    wbuf, lbuf, rbuf, acc, left, own, psend, precv, weight_ref, wother,
    xs, xr, ys, yr, zs, zr, fsend, frecv, load_sem, sems_s, sems_r, line_s, line_r, gat_s, gat_r,
):
    Z, X, T, K, rows, block, groups, orders = cfg
    half = block // 2
    pair, sector = lax.axis_index("pair"), lax.axis_index("sector")
    z, x = pair // X, lax.rem(pair, X)
    y, c = sector // 2, lax.rem(sector, 2)

    def dev(zz=None, xx=None, yy=None, cc=None):
        zz, xx = z if zz is None else zz, x if xx is None else xx
        yy, cc = y if yy is None else yy, c if cc is None else cc
        return (zz * X + xx, yy * 2 + cc)

    x_dev, y_dev, c_dev = dev(xx=1 - x), dev(yy=1 - y), dev(cc=1 - c)
    up_dev, dn_dev = dev(zz=z + 1), dev(zz=z - 1)

    def loop(count, f):
        def one(i, carry):
            f(i)
            return carry

        lax.fori_loop(0, count, one, 0)

    has_up, has_dn = z + 1 < Z, z >= 1

    loads = []
    for k in range(K):
        loads.append(pltpu.make_async_copy(left_hbm.at[k], lbuf.at[k], load_sem.at[k]))
        loads.append(pltpu.make_async_copy(right_hbm.at[k], rbuf.at[k], load_sem.at[K + k]))
    for k in range(K):
        loads[2 * k].start()

    barrier = pltpu.get_barrier_semaphore()
    for other in (x_dev, y_dev, c_dev):
        pl.semaphore_signal(barrier, inc=1, device_id=other, device_id_type=MESH)

    def greet(zz):
        @pl.when(zz != z)
        def _():
            pl.semaphore_signal(barrier, inc=1, device_id=dev(zz=zz), device_id_type=MESH)

    loop(Z, greet)
    size = sizes_ref[sector]
    row_ids = pair * rows + lax.broadcasted_iota(jnp.int32, (rows, LANES), 0)
    lane_ids = lax.broadcasted_iota(jnp.int32, (rows, LANES), 1)

    def used(column):
        return ((row_ids < size) & (lane_ids + column < size)).astype(F32)

    for at in range(0, block, LANES):
        value = wave_ref[:, at : at + LANES].astype(F32) * used(at)
        wbuf[z, x, :, at : at + LANES] = value.astype(jnp.bfloat16)
    for k in range(K):
        factor = coefs_ref[ids_ref[k]]
        for t in range(T):
            chosen = jnp.where(targets_ref[k, 0] == t, factor, 0.0)
            weight_ref[k * T + t] = jnp.full((8, LANES), chosen, F32)
    for g in range(groups):
        for tc in range(2):
            zr[g][tc, z] = jnp.zeros((rows, LANES), jnp.bfloat16)
    pl.semaphore_wait(barrier, 3 + Z - 1)

    def remote(src, dst, ss, rs, device):
        return pltpu.make_async_remote_copy(
            src_ref=src, dst_ref=dst, send_sem=ss, recv_sem=rs, device_id=device, device_id_type=MESH
        )

    piece = rows // PIECES if rows % (16 * PIECES) == 0 else rows
    pieces = rows // piece

    def block_at(q, xx, p):
        return wbuf.at[q, xx, pl.ds(p * piece, piece)]

    def hop(q, way, p):
        device = (up_dev, dn_dev, x_dev)[way]
        return remote(block_at(q, x, p), block_at(q, x, p), gat_s.at[way, q, p], gat_r.at[q, x, p], device)

    def arrival(q, xx, p):
        return remote(block_at(q, xx, p), block_at(q, xx, p), gat_s.at[2, q, p], gat_r.at[q, xx, p], x_dev)

    def pass_on(q, ways, p):
        if 0 in ways:
            @pl.when(has_up)
            def _():
                hop(q, 0, p).start()

        if 1 in ways:
            @pl.when(has_dn)
            def _():
                hop(q, 1, p).start()

        hop(q, 2, p).start()

    for p in range(pieces):
        pass_on(z, (0, 1), p)
    weights_copy = remote(weight_ref, wother, sems_s.at[0], sems_r.at[0], c_dev)
    weights_copy.start()
    for k in range(K):
        loads[2 * k + 1].start()

    depth = X * rows
    planewise = depth % PLANE_DEPTH == 0
    tile = min(ROW_TILE, block)
    tiles = block // tile

    def multiply(q, first):
        plane = wbuf.at[q]

        def one(i, carry):
            k, at = i // tiles, pl.multiple_of(lax.rem(i, tiles) * tile, tile)
            cols = pl.ds(pl.multiple_of(q * depth, depth), depth)
            product = jnp.dot(
                lbuf[k, pl.ds(at, tile), cols], plane[...].reshape(depth, block), preferred_element_type=F32
            )
            if first:
                acc[k, pl.ds(at, tile), :] = product
            else:
                acc[k, pl.ds(at, tile), :] += product
            return carry

        lax.fori_loop(0, K * tiles, one, 0)

    def take_plane(q, first=False):
        for p in range(pieces):
            arrival(q, 1 - x, p).wait_recv()
        if planewise:
            multiply(q, first)

    for k in range(K):
        loads[2 * k].wait()

    def forward(d, carry):
        lo, hi = z - d, z + d
        for p in range(pieces):
            @pl.when(lo >= 0)
            def _():
                arrival(lo, x, p).wait_recv()
                pass_on(lo, (0,), p)

            @pl.when(hi < Z)
            def _():
                arrival(hi, x, p).wait_recv()
                pass_on(hi, (1,), p)

        @pl.when(d == 1)
        def _():
            take_plane(z, True)

        return carry

    lax.fori_loop(1, Z, forward, 0)

    def take_planes(d, carry):
        @pl.when(z - d >= 0)
        def _():
            take_plane(z - d)

        @pl.when(z + d < Z)
        def _():
            take_plane(z + d)

        return carry

    lax.fori_loop(1, Z, take_planes, 0)

    def finish_left(i, carry):
        k, at = i // tiles, pl.multiple_of(lax.rem(i, tiles) * tile, tile)
        if planewise:
            value = acc[k, pl.ds(at, tile), :]
        else:
            value = jnp.dot(
                lbuf[k, pl.ds(at, tile), :], wbuf[...].reshape(block, block), preferred_element_type=F32
            )
        left[k, pl.ds(at, tile), :] = value.astype(jnp.bfloat16)
        return carry

    lax.fori_loop(0, K * tiles, finish_left, 0)
    for k in range(K):
        loads[2 * k + 1].wait()

    width = 2 * LANES

    def second(part, side, dest):
        def one(i, carry):
            k, at = i // tiles, pl.multiple_of(lax.rem(i, tiles) * tile, tile)
            right_at = pl.multiple_of(side * half + part * width, width)
            term = lax.dot_general(
                left[k, pl.ds(at, tile), :], rbuf[k, pl.ds(right_at, width), :],
                (((1,), (1,)), ((), ())), preferred_element_type=F32,
            )
            for j in range(2):
                dest[2 * part + j, k, pl.ds(at, tile), :] = term[:, j * LANES : (j + 1) * LANES].astype(dest.dtype)
            return carry

        lax.fori_loop(0, K * tiles, one, 0)

    def part_copy(part):
        span = pl.ds(2 * part, 2)
        return remote(psend.at[span], precv.at[span], sems_s.at[1 + part], sems_r.at[1 + part], c_dev)

    base = 1 + groups // 2

    def step_copy(g, number, tc):
        letter = orders[g][number]
        s, r = ((xs, xr), (ys, yr))["xy".index(letter)]
        at = base + 4 * g + 2 * number + tc
        return remote(s[g].at[tc], r[g].at[tc], sems_s.at[at], sems_r.at[at], x_dev if letter == "x" else y_dev)

    def chip_sum(g, ty, tc, zz, xx):
        at = pl.ds(pl.multiple_of((zz * X + xx) * rows, rows), rows)
        t = ty * 2 + tc
        total = None
        for k in range(K):
            mine = own[g, k, at, :] * weight_ref[k * T + t, 0:1, :]
            theirs = precv[g, k, at, :].astype(F32) * wother[k * T + t, 0:1, :]
            total = mine + theirs if total is None else total + mine + theirs
        return total

    def x_first(g, tc):
        def one(zz):
            for ty in range(2):
                xs[g][tc, ty, zz] = chip_sum(g, ty, tc, zz, 1 - x).astype(jnp.bfloat16)

        loop(Z, one)
        step_copy(g, 0, tc).start()

    def y_first(g, tc):
        def one(zz):
            for xx in range(2):
                ys[g][tc, zz, xx] = chip_sum(g, 1 - y, tc, zz, xx).astype(jnp.bfloat16)

        loop(Z, one)
        step_copy(g, 0, tc).start()

    def y_second(g, tc):
        step_copy(g, 0, tc).wait_recv()

        def one(zz):
            value = chip_sum(g, 1 - y, tc, zz, x) + xr[g][tc, 1 - y, zz].astype(F32)
            ys[g][tc, zz] = value.astype(jnp.bfloat16)

        loop(Z, one)
        step_copy(g, 1, tc).start()

    def x_second(g, tc):
        step_copy(g, 0, tc).wait_recv()

        def one(zz):
            value = chip_sum(g, y, tc, zz, 1 - x) + yr[g][tc, zz, 1 - x].astype(F32)
            xs[g][tc, zz] = value.astype(jnp.bfloat16)

        loop(Z, one)
        step_copy(g, 1, tc).start()

    def plane_sum(g, tc, zz):
        value = chip_sum(g, y, tc, zz, x)
        if orders[g][0] == "x":
            return value + xr[g][tc, y, zz].astype(F32) + yr[g][tc, zz].astype(F32)
        return value + yr[g][tc, zz, x].astype(F32) + xr[g][tc, zz].astype(F32)

    def line_copy(g, tc, zz):
        return remote(
            zs[g].at[tc, zz], zr[g].at[tc, z], line_s.at[g, tc, zz], line_r.at[g, tc, z], dev(zz=zz)
        )

    def line_arrival(g, tc, zz):
        return remote(
            zs[g].at[tc, zz], zr[g].at[tc, zz], line_s.at[g, tc, zz], line_r.at[g, tc, zz], dev(zz=zz)
        )

    def line(g, tc):
        step_copy(g, 1, tc).wait_recv()

        def one(j):
            zz = lax.rem(z + 1 + j, Z)
            zs[g][tc, zz] = plane_sum(g, tc, zz).astype(jnp.bfloat16)
            line_copy(g, tc, zz).start()

        loop(Z - 1, one)

    def total(g, tc):
        value = plane_sum(g, tc, z)
        if Z <= 8:
            for zz in range(Z):
                value = value + zr[g][tc, zz].astype(F32)
            return value
        return lax.fori_loop(0, Z, lambda zz, v: v + zr[g][tc, zz].astype(F32), value)

    def final_copy(g):
        at = base + 4 * groups + g
        return remote(fsend.at[g], frecv.at[g], sems_s.at[at], sems_r.at[at], c_dev)

    def finish(g):
        def wait(j):
            for tc in range(2):
                line_arrival(g, tc, lax.rem(z + 1 + j, Z)).wait_recv()

        loop(Z - 1, wait)
        fsend[g] = total(g, 1 - c)
        final_copy(g).start()
        at = pl.multiple_of(c * half + g * LANES, LANES)
        out_ref[:, pl.ds(at, LANES)] = total(g, c) * used(at)

    def first(i):
        x_first(2 * (i // 2), i % 2)
        y_first(2 * (i // 2) + 1, i % 2)

    def next_step(i):
        y_second(2 * (i // 2), i % 2)
        x_second(2 * (i // 2) + 1, i % 2)

    def lines(i):
        line(2 * (i // 2), i % 2)
        line(2 * (i // 2) + 1, i % 2)

    parts = groups // 2
    rounds = groups
    second(0, 1 - c, psend)
    part_copy(0).start()
    second(0, c, own)
    weights_copy.wait_recv()
    for i in range(rounds):
        part = i // 2
        if i % 2 == 0:
            if part + 1 < parts:
                second(part + 1, 1 - c, psend)
                part_copy(part + 1).start()
            part_copy(part).wait_recv()
        first(i)
        if i % 2 == 1 and part + 1 < parts:
            second(part + 1, c, own)
        if i >= 1:
            next_step(i - 1)
        if i >= 2:
            lines(i - 2)
    next_step(rounds - 1)
    lines(rounds - 2)
    for g in range(groups - 2):
        finish(g)
    lines(rounds - 1)
    for g in range(groups - 2, groups):
        finish(g)
    for g in range(groups):
        final_copy(g).wait_recv()
        at = pl.multiple_of((1 - c) * half + g * LANES, LANES)
        out_ref[:, pl.ds(at, LANES)] = frecv[g] * used(at)

    def drain(q):
        for p in range(pieces):
            @pl.when(jnp.logical_and(has_up, q <= z))
            def _():
                hop(q, 0, p).wait_send()

            @pl.when(jnp.logical_and(has_dn, q >= z))
            def _():
                hop(q, 1, p).wait_send()

            hop(q, 2, p).wait_send()

    loop(Z, drain)
    weights_copy.wait_send()
    for part in range(parts):
        part_copy(part).wait_send()
    for g in range(groups):
        final_copy(g).wait_send()
        for tc in range(2):
            step_copy(g, 0, tc).wait_send()
            step_copy(g, 1, tc).wait_send()

            def drain_line(j, g=g, tc=tc):
                line_copy(g, tc, lax.rem(z + 1 + j, Z)).wait_send()

            loop(Z - 1, drain_line)


def kernel_entry(cfg, *refs):
    groups = cfg[6]
    ins, scratch = refs[:8], list(refs[8:])
    plain = scratch[:10]
    per_group = [scratch[10 + n * groups : 10 + (n + 1) * groups] for n in range(6)]
    step_kernel(cfg, *ins, *plain, *per_group, *scratch[10 + 6 * groups :])


def body(wave, left_ops, right_ops, targets, sector_sizes, pair_ids, pair_coefficients):
    block = wave.shape[2]
    rows = wave.shape[1]
    K = left_ops.shape[0]
    T = sector_sizes.shape[0]
    pairs = lax.axis_size("pair")
    X = 2
    Z = pairs // X
    half = block // 2
    groups = half // LANES
    orders = tuple(("xyz", "yxz")[g % 2] for g in range(groups))
    bf = jnp.bfloat16
    xs, xr, ys, yr, zs, zr = [], [], [], [], [], []
    for order in orders:
        tail = (rows, LANES)
        x_shape, y_shape = {"x": ((2, 2, Z), (2, Z)), "y": ((2, Z), (2, Z, X))}[order[0]]
        for where, shape in ((xs, x_shape), (xr, x_shape), (ys, y_shape), (yr, y_shape), (zs, (2, Z)), (zr, (2, Z))):
            where.append(pltpu.VMEM(shape + tail, bf))
    count = 1 + groups // 2 + 5 * groups
    dma = pltpu.SemaphoreType.DMA
    cfg = (Z, X, T, K, rows, block, groups, orders)
    planewise = (X * rows) % PLANE_DEPTH == 0
    vmem, anywhere = pl.BlockSpec(memory_space=pltpu.VMEM), pl.BlockSpec(memory_space=pl.ANY)
    smem = pl.BlockSpec(memory_space=pltpu.SMEM)
    out = pl.pallas_call(
        functools.partial(kernel_entry, cfg),
        out_shape=jax.ShapeDtypeStruct((rows, block), F32),
        in_specs=[vmem, smem, smem, smem, smem, anywhere, anywhere],
        out_specs=vmem,
        scratch_shapes=[
            pltpu.VMEM((Z, X, rows, block), bf),
            pltpu.VMEM((K, block, block), bf),
            pltpu.VMEM((K, block, block), bf),
            pltpu.VMEM((K, block, block) if planewise else (8, LANES), F32),
            pltpu.VMEM((K, block, block), bf),
            pltpu.VMEM((groups, K, block, LANES), F32),
            pltpu.VMEM((groups, K, block, LANES), F32),
            pltpu.VMEM((groups, K, block, LANES), F32),
            pltpu.VMEM((K * T, 8, LANES), F32),
            pltpu.VMEM((K * T, 8, LANES), F32),
            *xs, *xr, *ys, *yr, *zs, *zr,
            pltpu.VMEM((groups, rows, LANES), F32),
            pltpu.VMEM((groups, rows, LANES), F32),
            dma((2 * K,)), dma((count,)), dma((count,)),
            dma((groups, 2, Z)), dma((groups, 2, Z)), dma((3, Z, PIECES)), dma((Z, X, PIECES)),
        ],
        compiler_params=pltpu.CompilerParams(
            collective_id=0, has_side_effects=True, vmem_limit_bytes=60 * 1024 * 1024
        ),
        name="sigma_step",
    )(wave[0], targets, sector_sizes, pair_ids, pair_coefficients, left_ops[:, 0], right_ops[:, 0])
    return out[None]


def solution(mesh):
    placed = (
        P("sector", "pair", None),
        P("pair", "sector", None, None),
        P("pair", "sector", None, None),
        P("pair", "sector"),
        P(),
        P("pair"),
        P(),
    )
    return jax.shard_map(
        body, mesh=mesh, in_specs=placed, out_specs=P("sector", "pair", None), check_vma=False
    )
```

```python
import functools

import jax
import jax.numpy as jnp
from jax import lax
from jax.experimental import pallas as pl
from jax.experimental.pallas import tpu as pltpu
from jax.sharding import PartitionSpec as P

MESH = pl.DeviceIdType.MESH
F32 = jnp.float32
LANES = 128
PLANE_DEPTH = 128
ROW_TILE = 512
PIECES = 2


def step_kernel(
    cfg, wave_ref, targets_ref, sizes_ref, ids_ref, coefs_ref, left_hbm, right_hbm, out_ref,
    wbuf, lbuf, rbuf, acc, left, own, psend, precv, weight_ref, wother,
    xs, xr, ys, yr, zs, zr, fsend, frecv, load_sem, sems_s, sems_r, line_s, line_r, gat_s, gat_r,
):
    Z, X, T, K, rows, block, groups, orders = cfg
    half = block // 2
    pair, sector = lax.axis_index("pair"), lax.axis_index("sector")
    z, x = pair // X, lax.rem(pair, X)
    y, c = sector // 2, lax.rem(sector, 2)

    def dev(zz=None, xx=None, yy=None, cc=None):
        zz, xx = z if zz is None else zz, x if xx is None else xx
        yy, cc = y if yy is None else yy, c if cc is None else cc
        return (zz * X + xx, yy * 2 + cc)

    x_dev, y_dev, c_dev = dev(xx=1 - x), dev(yy=1 - y), dev(cc=1 - c)
    up_dev, dn_dev = dev(zz=z + 1), dev(zz=z - 1)

    def loop(count, f):
        def one(i, carry):
            f(i)
            return carry

        lax.fori_loop(0, count, one, 0)

    has_up, has_dn = z + 1 < Z, z >= 1

    loads = []
    for k in range(K):
        loads.append(pltpu.make_async_copy(left_hbm.at[k], lbuf.at[k], load_sem.at[k]))
        loads.append(pltpu.make_async_copy(right_hbm.at[k], rbuf.at[k], load_sem.at[K + k]))
    for k in range(K):
        loads[2 * k].start()

    barrier = pltpu.get_barrier_semaphore()
    for other in (x_dev, y_dev, c_dev):
        pl.semaphore_signal(barrier, inc=1, device_id=other, device_id_type=MESH)

    def greet(zz):
        @pl.when(zz != z)
        def _():
            pl.semaphore_signal(barrier, inc=1, device_id=dev(zz=zz), device_id_type=MESH)

    loop(Z, greet)
    size = sizes_ref[sector]
    row_ids = pair * rows + lax.broadcasted_iota(jnp.int32, (rows, LANES), 0)
    lane_ids = lax.broadcasted_iota(jnp.int32, (rows, LANES), 1)

    def used(column):
        return ((row_ids < size) & (lane_ids + column < size)).astype(F32)

    for at in range(0, block, LANES):
        value = wave_ref[:, at : at + LANES].astype(F32) * used(at)
        wbuf[z, x, :, at : at + LANES] = value.astype(jnp.bfloat16)
    for k in range(K):
        factor = coefs_ref[ids_ref[k]]
        for t in range(T):
            chosen = jnp.where(targets_ref[k, 0] == t, factor, 0.0)
            weight_ref[k * T + t] = jnp.full((8, LANES), chosen, F32)
    for g in range(groups):
        for tc in range(2):
            zr[g][tc, z] = jnp.zeros((rows, LANES), jnp.bfloat16)
    pl.semaphore_wait(barrier, 3 + Z - 1)

    def remote(src, dst, ss, rs, device):
        return pltpu.make_async_remote_copy(
            src_ref=src, dst_ref=dst, send_sem=ss, recv_sem=rs, device_id=device, device_id_type=MESH
        )

    piece = rows // PIECES if rows % (16 * PIECES) == 0 else rows
    pieces = rows // piece

    def block_at(q, xx, p):
        return wbuf.at[q, xx, pl.ds(p * piece, piece)]

    def hop(q, way, p):
        device = (up_dev, dn_dev, x_dev)[way]
        return remote(block_at(q, x, p), block_at(q, x, p), gat_s.at[way, q, p], gat_r.at[q, x, p], device)

    def arrival(q, xx, p):
        return remote(block_at(q, xx, p), block_at(q, xx, p), gat_s.at[2, q, p], gat_r.at[q, xx, p], x_dev)

    def pass_on(q, ways, p):
        if 0 in ways:
            @pl.when(has_up)
            def _():
                hop(q, 0, p).start()

        if 1 in ways:
            @pl.when(has_dn)
            def _():
                hop(q, 1, p).start()

        hop(q, 2, p).start()

    for p in range(pieces):
        pass_on(z, (0, 1), p)
    weights_copy = remote(weight_ref, wother, sems_s.at[0], sems_r.at[0], c_dev)
    weights_copy.start()
    for k in range(K):
        loads[2 * k + 1].start()

    depth = X * rows
    planewise = depth % PLANE_DEPTH == 0
    tile = min(ROW_TILE, block)
    tiles = block // tile

    def multiply(q, first):
        plane = wbuf.at[q]

        def one(i, carry):
            k, at = i // tiles, pl.multiple_of(lax.rem(i, tiles) * tile, tile)
            cols = pl.ds(pl.multiple_of(q * depth, depth), depth)
            product = jnp.dot(
                lbuf[k, pl.ds(at, tile), cols], plane[...].reshape(depth, block), preferred_element_type=F32
            )
            if first:
                acc[k, pl.ds(at, tile), :] = product
            else:
                acc[k, pl.ds(at, tile), :] += product
            return carry

        lax.fori_loop(0, K * tiles, one, 0)

    def take_plane(q, first=False):
        for p in range(pieces):
            arrival(q, 1 - x, p).wait_recv()
        if planewise:
            multiply(q, first)

    for k in range(K):
        loads[2 * k].wait()

    def forward(d, carry):
        lo, hi = z - d, z + d
        for p in range(pieces):
            @pl.when(lo >= 0)
            def _():
                arrival(lo, x, p).wait_recv()
                pass_on(lo, (0,), p)

            @pl.when(hi < Z)
            def _():
                arrival(hi, x, p).wait_recv()
                pass_on(hi, (1,), p)

        @pl.when(d == 1)
        def _():
            take_plane(z, True)

        return carry

    lax.fori_loop(1, Z, forward, 0)

    def take_planes(d, carry):
        @pl.when(z - d >= 0)
        def _():
            take_plane(z - d)

        @pl.when(z + d < Z)
        def _():
            take_plane(z + d)

        return carry

    lax.fori_loop(1, Z, take_planes, 0)

    def finish_left(i, carry):
        k, at = i // tiles, pl.multiple_of(lax.rem(i, tiles) * tile, tile)
        if planewise:
            value = acc[k, pl.ds(at, tile), :]
        else:
            value = jnp.dot(
                lbuf[k, pl.ds(at, tile), :], wbuf[...].reshape(block, block), preferred_element_type=F32
            )
        left[k, pl.ds(at, tile), :] = value.astype(jnp.bfloat16)
        return carry

    lax.fori_loop(0, K * tiles, finish_left, 0)
    for k in range(K):
        loads[2 * k + 1].wait()

    width = 2 * LANES

    def second(part, side, dest):
        def one(i, carry):
            k, at = i // tiles, pl.multiple_of(lax.rem(i, tiles) * tile, tile)
            right_at = pl.multiple_of(side * half + part * width, width)
            term = lax.dot_general(
                left[k, pl.ds(at, tile), :], rbuf[k, pl.ds(right_at, width), :],
                (((1,), (1,)), ((), ())), preferred_element_type=F32,
            )
            for j in range(2):
                dest[2 * part + j, k, pl.ds(at, tile), :] = term[:, j * LANES : (j + 1) * LANES].astype(dest.dtype)
            return carry

        lax.fori_loop(0, K * tiles, one, 0)

    def part_copy(part):
        span = pl.ds(2 * part, 2)
        return remote(psend.at[span], precv.at[span], sems_s.at[1 + part], sems_r.at[1 + part], c_dev)

    base = 1 + groups // 2

    def step_copy(g, number, tc):
        letter = orders[g][number]
        s, r = ((xs, xr), (ys, yr))["xy".index(letter)]
        at = base + 4 * g + 2 * number + tc
        return remote(s[g].at[tc], r[g].at[tc], sems_s.at[at], sems_r.at[at], x_dev if letter == "x" else y_dev)

    def chip_sum(g, ty, tc, zz, xx):
        at = pl.ds(pl.multiple_of((zz * X + xx) * rows, rows), rows)
        t = ty * 2 + tc
        total = None
        for k in range(K):
            mine = own[g, k, at, :] * weight_ref[k * T + t, 0:1, :]
            theirs = precv[g, k, at, :].astype(F32) * wother[k * T + t, 0:1, :]
            total = mine + theirs if total is None else total + mine + theirs
        return total

    def x_first(g, tc):
        def one(zz):
            for ty in range(2):
                xs[g][tc, ty, zz] = chip_sum(g, ty, tc, zz, 1 - x).astype(jnp.bfloat16)

        loop(Z, one)
        step_copy(g, 0, tc).start()

    def y_first(g, tc):
        def one(zz):
            for xx in range(2):
                ys[g][tc, zz, xx] = chip_sum(g, 1 - y, tc, zz, xx).astype(jnp.bfloat16)

        loop(Z, one)
        step_copy(g, 0, tc).start()

    def y_second(g, tc):
        step_copy(g, 0, tc).wait_recv()

        def one(zz):
            value = chip_sum(g, 1 - y, tc, zz, x) + xr[g][tc, 1 - y, zz].astype(F32)
            ys[g][tc, zz] = value.astype(jnp.bfloat16)

        loop(Z, one)
        step_copy(g, 1, tc).start()

    def x_second(g, tc):
        step_copy(g, 0, tc).wait_recv()

        def one(zz):
            value = chip_sum(g, y, tc, zz, 1 - x) + yr[g][tc, zz, 1 - x].astype(F32)
            xs[g][tc, zz] = value.astype(jnp.bfloat16)

        loop(Z, one)
        step_copy(g, 1, tc).start()

    def plane_sum(g, tc, zz):
        value = chip_sum(g, y, tc, zz, x)
        if orders[g][0] == "x":
            return value + xr[g][tc, y, zz].astype(F32) + yr[g][tc, zz].astype(F32)
        return value + yr[g][tc, zz, x].astype(F32) + xr[g][tc, zz].astype(F32)

    def line_copy(g, tc, zz):
        return remote(
            zs[g].at[tc, zz], zr[g].at[tc, z], line_s.at[g, tc, zz], line_r.at[g, tc, z], dev(zz=zz)
        )

    def line_arrival(g, tc, zz):
        return remote(
            zs[g].at[tc, zz], zr[g].at[tc, zz], line_s.at[g, tc, zz], line_r.at[g, tc, zz], dev(zz=zz)
        )

    def line(g, tc):
        step_copy(g, 1, tc).wait_recv()

        def one(j):
            zz = lax.rem(z + 1 + j, Z)
            zs[g][tc, zz] = plane_sum(g, tc, zz).astype(jnp.bfloat16)
            line_copy(g, tc, zz).start()

        loop(Z - 1, one)

    def total(g, tc):
        value = plane_sum(g, tc, z)
        if Z <= 8:
            for zz in range(Z):
                value = value + zr[g][tc, zz].astype(F32)
            return value
        return lax.fori_loop(0, Z, lambda zz, v: v + zr[g][tc, zz].astype(F32), value)

    def final_copy(g):
        at = base + 4 * groups + g
        return remote(fsend.at[g], frecv.at[g], sems_s.at[at], sems_r.at[at], c_dev)

    def finish(g):
        def wait(j):
            for tc in range(2):
                line_arrival(g, tc, lax.rem(z + 1 + j, Z)).wait_recv()

        loop(Z - 1, wait)
        fsend[g] = total(g, 1 - c)
        final_copy(g).start()
        at = pl.multiple_of(c * half + g * LANES, LANES)
        out_ref[:, pl.ds(at, LANES)] = total(g, c) * used(at)

    def first(i):
        x_first(2 * (i // 2), i % 2)
        y_first(2 * (i // 2) + 1, i % 2)

    def next_step(i):
        y_second(2 * (i // 2), i % 2)
        x_second(2 * (i // 2) + 1, i % 2)

    def lines(i):
        line(2 * (i // 2), i % 2)
        line(2 * (i // 2) + 1, i % 2)

    parts = groups // 2
    rounds = groups
    second(0, 1 - c, psend)
    part_copy(0).start()
    second(0, c, own)
    weights_copy.wait_recv()
    for i in range(rounds):
        part = i // 2
        if i % 2 == 0:
            if part + 1 < parts:
                second(part + 1, 1 - c, psend)
                part_copy(part + 1).start()
            part_copy(part).wait_recv()
        first(i)
        if i % 2 == 1 and part + 1 < parts:
            second(part + 1, c, own)
        if i >= 1:
            next_step(i - 1)
        if i >= 2:
            lines(i - 2)
    next_step(rounds - 1)
    lines(rounds - 2)
    for g in range(groups - 2):
        finish(g)
    lines(rounds - 1)
    for g in range(groups - 2, groups):
        finish(g)
    for g in range(groups):
        final_copy(g).wait_recv()
        at = pl.multiple_of((1 - c) * half + g * LANES, LANES)
        out_ref[:, pl.ds(at, LANES)] = frecv[g] * used(at)

    def drain(q):
        for p in range(pieces):
            @pl.when(jnp.logical_and(has_up, q <= z))
            def _():
                hop(q, 0, p).wait_send()

            @pl.when(jnp.logical_and(has_dn, q >= z))
            def _():
                hop(q, 1, p).wait_send()

            hop(q, 2, p).wait_send()

    loop(Z, drain)
    weights_copy.wait_send()
    for part in range(parts):
        part_copy(part).wait_send()
    for g in range(groups):
        final_copy(g).wait_send()
        for tc in range(2):
            step_copy(g, 0, tc).wait_send()
            step_copy(g, 1, tc).wait_send()

            def drain_line(j, g=g, tc=tc):
                line_copy(g, tc, lax.rem(z + 1 + j, Z)).wait_send()

            loop(Z - 1, drain_line)


def kernel_entry(cfg, *refs):
    groups = cfg[6]
    ins, scratch = refs[:8], list(refs[8:])
    plain = scratch[:10]
    per_group = [scratch[10 + n * groups : 10 + (n + 1) * groups] for n in range(6)]
    step_kernel(cfg, *ins, *plain, *per_group, *scratch[10 + 6 * groups :])


def body(wave, left_ops, right_ops, targets, sector_sizes, pair_ids, pair_coefficients):
    block = wave.shape[2]
    rows = wave.shape[1]
    K = left_ops.shape[0]
    T = sector_sizes.shape[0]
    pairs = lax.axis_size("pair")
    X = 2
    Z = pairs // X
    half = block // 2
    groups = half // LANES
    orders = tuple(("xyz", "yxz")[g % 2] for g in range(groups))
    bf = jnp.bfloat16
    xs, xr, ys, yr, zs, zr = [], [], [], [], [], []
    for order in orders:
        tail = (rows, LANES)
        x_shape, y_shape = {"x": ((2, 2, Z), (2, Z)), "y": ((2, Z), (2, Z, X))}[order[0]]
        for where, shape in ((xs, x_shape), (xr, x_shape), (ys, y_shape), (yr, y_shape), (zs, (2, Z)), (zr, (2, Z))):
            where.append(pltpu.VMEM(shape + tail, bf))
    count = 1 + groups // 2 + 5 * groups
    dma = pltpu.SemaphoreType.DMA
    cfg = (Z, X, T, K, rows, block, groups, orders)
    planewise = (X * rows) % PLANE_DEPTH == 0
    vmem, anywhere = pl.BlockSpec(memory_space=pltpu.VMEM), pl.BlockSpec(memory_space=pl.ANY)
    smem = pl.BlockSpec(memory_space=pltpu.SMEM)
    out = pl.pallas_call(
        functools.partial(kernel_entry, cfg),
        out_shape=jax.ShapeDtypeStruct((rows, block), F32),
        in_specs=[vmem, smem, smem, smem, smem, anywhere, anywhere],
        out_specs=vmem,
        scratch_shapes=[
            pltpu.VMEM((Z, X, rows, block), bf),
            pltpu.VMEM((K, block, block), bf),
            pltpu.VMEM((K, block, block), bf),
            pltpu.VMEM((K, block, block) if planewise else (8, LANES), F32),
            pltpu.VMEM((K, block, block), bf),
            pltpu.VMEM((groups, K, block, LANES), F32),
            pltpu.VMEM((groups, K, block, LANES), F32),
            pltpu.VMEM((groups, K, block, LANES), F32),
            pltpu.VMEM((K * T, 8, LANES), F32),
            pltpu.VMEM((K * T, 8, LANES), F32),
            *xs, *xr, *ys, *yr, *zs, *zr,
            pltpu.VMEM((groups, rows, LANES), F32),
            pltpu.VMEM((groups, rows, LANES), F32),
            dma((2 * K,)), dma((count,)), dma((count,)),
            dma((groups, 2, Z)), dma((groups, 2, Z)), dma((3, Z, PIECES)), dma((Z, X, PIECES)),
        ],
        compiler_params=pltpu.CompilerParams(
            collective_id=0, has_side_effects=True, vmem_limit_bytes=60 * 1024 * 1024
        ),
        name="sigma_step",
    )(wave[0], targets, sector_sizes, pair_ids, pair_coefficients, left_ops[:, 0], right_ops[:, 0])
    return out[None]


def solution(mesh):
    placed = (
        P("sector", "pair", None),
        P("pair", "sector", None, None),
        P("pair", "sector", None, None),
        P("pair", "sector"),
        P(),
        P("pair"),
        P(),
    )
    return jax.shard_map(
        body, mesh=mesh, in_specs=placed, out_specs=P("sector", "pair", None), check_vma=False
    )
```
